32 devices in a mesh: gx: 2 (over x), gy: 4 (over z), gz: 4 (over y, core).
Axes of the slice: x: 2, y: 2, z: 4, core: 2. Of those that a mesh axis runs over, the one named last changes fastest.
Arguments:
- body_load: float32 [3, 8, 64, 512], P(None, 'gx', 'gy', 'gz'), may hold values from -24 to 24
- contact_mask: int32 [8, 64, 512], P('gx', 'gy', 'gz'), may hold values 0 or 1
- contact_gap: float32 [8, 64, 512], P('gx', 'gy', 'gz'), may hold values from 0.1 to 0.8
- material_ids: int32 [8, 64, 512], P('gx', 'gy', 'gz'), may hold values from 0 to 3
- lame_table: float32 [4, 2], replicated, may hold values from 0.5 to 2
Outputs:
- displacement: float32 [3, 8, 64, 512], P(None, 'gx', 'gy', 'gz')
- multiplier: float32 [3, 8, 64, 512], P(None, 'gx', 'gy', 'gz')
- gap_history: float32 [6], replicated
The draws below stay inside these ranges and needn't reach their ends.
All inputs are finite; a program needn't handle non-finite values. No bound on the sum of `contact_mask` on one device may be relied on, other than what follows from the above.
Results may differ from the reference program's by a relative error of at most 0.0001.
Values sent between devices are 32-bit elements; how exact they have to be, the bound alone decides.
A program may use at most 64 MiB of HBM per device.

```python
import math
import jax
import jax.numpy as jnp
import numpy as np
from jax import lax

CX = 4
ITERS = 6
NMAT = 4
NX = 8
NY = 64
NZ = 512


def place_ends(values, stream_key, low, high):
    place = [jax.random.randint(jax.random.fold_in(stream_key, axis), (), 0, length) for axis, length in enumerate(values.shape)]
    longest = values.shape.index(max(values.shape))
    neighbour = place[:longest] + [(place[longest] + 1) % values.shape[longest]] + place[longest + 1:]
    return values.at[tuple(place)].set(low).at[tuple(neighbour)].set(high)


def shard_levels(key, dims, cuts, least, top_value):
    level, own = 1.0, jax.random.fold_in(key, 6)
    for dim, shards_of in cuts:
        draws = jnp.exp(jax.random.uniform(jax.random.fold_in(own, dim), (shards_of,), jnp.float32, least / len(cuts), top_value / len(cuts)))
        level = level * jnp.repeat(draws, dims[dim] // shards_of).reshape([-1 if axis == dim else 1 for axis in range(len(dims))])
    return level


def noise(stream_key, dims, scale, limit, cuts=(), kind=jnp.bfloat16):
    values = jax.random.normal(stream_key, dims, jnp.float32) * scale
    if len(cuts) > 0:
        values = shard_levels(stream_key, dims, cuts, -0.22, 0.18) * values
    return jnp.clip(values, min=-limit, max=limit).astype(kind)


def setup_inputs(seed: int = 0) -> dict:
    arg_keys = jax.random.split(jax.random.key(seed), 6)
    return {
        "body_load": noise(arg_keys[0], (3, NX, NY, NZ), 4.0, 24.0, ((1, 2), (2, 4), (3, 4)), jnp.float32),
        "contact_mask": place_ends((jax.random.randint(arg_keys[1], (NX, NY, NZ), 0, 3) < 1).astype(jnp.int32), jax.random.fold_in(arg_keys[1], 1), 0, 1),
        "contact_gap": jnp.clip(0.1 + 0.7 * jax.random.uniform(arg_keys[2], (NX, NY, NZ), jnp.float32) ** shard_levels(arg_keys[2], (NX, NY, NZ), ((0, 2), (1, 4), (2, 4)), -0.2, 0.2), 0.1, 0.8),
        "material_ids": place_ends(jax.random.randint(arg_keys[3], (NX, NY, NZ), 0, NMAT), jax.random.fold_in(arg_keys[3], 1), 0, NMAT - 1).astype(jnp.int32),
        "lame_table": jnp.clip(jnp.exp(jax.random.uniform(arg_keys[4], (NMAT, 2), jnp.float32, math.log(0.5), math.log(2.0))), 0.5, 2.0),
    }


def corner_offsets(a):
    return ((a >> 2) & 1, (a >> 1) & 1, a & 1)


def element_tables():
    points = np.array([(1.0 - 3.0 ** -0.5) / 2.0, (1.0 + 3.0 ** -0.5) / 2.0])
    stiff_lame = np.zeros((24, 24))
    stiff_shear = np.zeros((24, 24))
    for p in points:
        for q in points:
            for r in points:
                position = (p, q, r)
                gradients = np.zeros((8, 3))
                for a in range(8):
                    corner = corner_offsets(a)
                    for d in range(3):
                        factor = 1.0
                        for e in range(3):
                            if e == d:
                                factor = factor * (1.0 if corner[e] else -1.0)
                            else:
                                factor = factor * (position[e] if corner[e] else 1.0 - position[e])
                        gradients[a, d] = factor
                for a in range(8):
                    for c in range(3):
                        for b in range(8):
                            for d in range(3):
                                stiff_lame[3 * a + c, 3 * b + d] += 0.125 * gradients[a, c] * gradients[b, d]
                                stiff_shear[3 * a + c, 3 * b + d] += 0.125 * (float(c == d) * np.dot(gradients[a], gradients[b]) + gradients[a, d] * gradients[b, c])
    return stiff_lame, stiff_shear


def material_fields(material_ids, lame_table):
    first = jnp.zeros(material_ids.shape, jnp.float32)
    shear = jnp.zeros(material_ids.shape, jnp.float32)
    for m in range(lame_table.shape[0]):
        hit = material_ids == m
        first = jnp.where(hit, lame_table[m, 0], first)
        shear = jnp.where(hit, lame_table[m, 1], shear)
    return first, shear


def element_forces(nodes, first, shear, kboth, counts):
    ecx, ecy, ecz = counts
    corners = []
    for a in range(8):
        o = corner_offsets(a)
        corners.append(nodes[:, o[0]:o[0] + ecx, o[1]:o[1] + ecy, o[2]:o[2] + ecz])
    stacked = jnp.stack(corners, 0).reshape(24, ecx * ecy * ecz)
    product = jnp.dot(kboth, stacked, precision=lax.Precision.HIGHEST, preferred_element_type=jnp.float32)
    result = first[:ecx, :ecy, :ecz].reshape(-1) * product[:24] + shear[:ecx, :ecy, :ecz].reshape(-1) * product[24:]
    return result.reshape(8, 3, ecx, ecy, ecz)


def assemble(forces, counts):
    ncx, ncy, ncz = counts
    total = None
    for a in range(8):
        o = corner_offsets(a)
        piece = forces[a][:, 1 - o[0]:1 - o[0] + ncx, 1 - o[1]:1 - o[1] + ncy, 1 - o[2]:1 - o[2] + ncz]
        total = piece if total is None else total + piece
    return total


def reference(body_load, contact_mask, contact_gap, material_ids, lame_table):
    stiff_lame, stiff_shear = element_tables()
    kboth = jnp.asarray(np.concatenate([stiff_lame, stiff_shear], 0), jnp.float32)
    lame_rows = float(np.max(np.sum(np.abs(stiff_lame), 1)))
    shear_rows = float(np.max(np.sum(np.abs(stiff_shear), 1)))
    bound = 8.0 * jnp.max(lame_table[:, 0] * lame_rows + lame_table[:, 1] * shear_rows)
    step_size = 1.5 / (1.0 + bound)
    first, shear = material_fields(material_ids, lame_table)
    first_ext = jnp.pad(first, ((1, 0), (1, 0), (1, 0)), mode="wrap")
    shear_ext = jnp.pad(shear, ((1, 0), (1, 0), (1, 0)), mode="wrap")
    slab = CX
    starts = jnp.arange(NX // slab, dtype=jnp.int32) * slab

    def apply_stiffness(displace):
        padded = jnp.pad(displace, ((0, 0), (1, 1), (1, 1), (1, 1)), mode="wrap")

        def one_slab(start):
            zero = jnp.zeros((), jnp.int32)
            nodes = lax.dynamic_slice(padded, (zero, start, zero, zero), (3, slab + 2, NY + 2, NZ + 2))
            first_slab = lax.dynamic_slice(first_ext, (start, zero, zero), (slab + 1, NY + 1, NZ + 1))
            shear_slab = lax.dynamic_slice(shear_ext, (start, zero, zero), (slab + 1, NY + 1, NZ + 1))
            forces = element_forces(nodes, first_slab, shear_slab, kboth, (slab + 1, NY + 1, NZ + 1))
            return assemble(forces, (slab, NY, NZ))

        stacked = lax.map(one_slab, starts)
        return jnp.moveaxis(stacked, 0, 1).reshape(3, NX, NY, NZ)

    primal = jnp.zeros(body_load.shape, jnp.float32)
    split = jnp.zeros(body_load.shape, jnp.float32)
    scaled_dual = jnp.zeros(body_load.shape, jnp.float32)
    history = []
    for t in range(ITERS):
        forces = apply_stiffness(primal)
        primal = primal - step_size * (forces - body_load + (primal - split + scaled_dual))
        shifted = primal + scaled_dual
        bounded = jnp.where(contact_mask > 0, jnp.maximum(shifted[2], -contact_gap), shifted[2])
        split = jnp.concatenate([shifted[:2], bounded[None]], 0)
        scaled_dual = shifted - split
        history.append(jnp.max(jnp.abs(primal - split)))
    return primal, scaled_dual, jnp.stack(history)
```

```python
import functools

import jax
import jax.numpy as jnp
import numpy as np
from jax import lax
from jax.experimental import pallas as pl
from jax.experimental.pallas import tpu as pltpu
from jax.sharding import PartitionSpec as P

ITERS = 6
DEPTHS = (1, 1, 1, 1, 1)
AXES = ("gx", "gy", "gz")
MESH = pl.DeviceIdType.MESH
DIRS = [
    (dx, dy, dz) for dx in (-1, 0, 1) for dy in (-1, 0, 1) for dz in (-1, 0, 1) if (dx, dy, dz) != (0, 0, 0)
]
DIRS.sort(key=lambda k: -sum(abs(a) for a in k))


def corner_offsets(a):
    return (a >> 2 & 1, a >> 1 & 1, a & 1)


def element_tables():
    points = np.array([(1.0 - 3.0 ** (-0.5)) / 2.0, (1.0 + 3.0 ** (-0.5)) / 2.0])
    stiff_lame = np.zeros((24, 24))
    stiff_shear = np.zeros((24, 24))
    for p in points:
        for q in points:
            for r in points:
                position = (p, q, r)
                gradients = np.zeros((8, 3))
                for a in range(8):
                    corner = corner_offsets(a)
                    for d in range(3):
                        factor = 1.0
                        for e in range(3):
                            if e == d:
                                factor = factor * (1.0 if corner[e] else -1.0)
                            else:
                                factor = factor * (position[e] if corner[e] else 1.0 - position[e])
                        gradients[a, d] = factor
                for a in range(8):
                    for c in range(3):
                        for b in range(8):
                            for d in range(3):
                                stiff_lame[3 * a + c, 3 * b + d] += 0.125 * gradients[a, c] * gradients[b, d]
                                stiff_shear[3 * a + c, 3 * b + d] += 0.125 * (
                                    float(c == d) * np.dot(gradients[a], gradients[b])
                                    + gradients[a, d] * gradients[b, c]
                                )
    return (stiff_lame, stiff_shear)


def element_modes(m, L, M):
    x, y, z = m
    M2 = M + M
    L3 = L * (1.0 / 3.0)
    M3 = M * (1.0 / 3.0)
    Q = (L + (M2 + M2)) * (1.0 / 9.0)
    s = L * (x["DSS"] + y["SDS"] + z["SSD"])
    fx, fy, fz = {}, {}, {}
    fx["DSS"] = s + M2 * x["DSS"]
    fy["SDS"] = s + M2 * y["SDS"]
    fz["SSD"] = s + M2 * z["SSD"]
    fy["DSS"] = fx["SDS"] = M * (y["DSS"] + x["SDS"])
    fz["DSS"] = fx["SSD"] = M * (z["DSS"] + x["SSD"])
    fz["SDS"] = fy["SSD"] = M * (z["SDS"] + y["SSD"])
    ax = L3 * (y["DDS"] + z["DSD"])
    ay = L3 * (x["DDS"] + z["SDD"])
    az = L3 * (x["DSD"] + y["SDD"])
    fx["DDS"] = ay + M * x["DDS"]
    fx["DSD"] = az + M * x["DSD"]
    fy["DDS"] = ax + M * y["DDS"]
    fy["SDD"] = az + M * y["SDD"]
    fz["DSD"] = ax + M * z["DSD"]
    fz["SDD"] = ay + M * z["SDD"]
    p = M3 * (y["DSD"] + x["SDD"])
    q = M3 * (x["SDD"] + z["DDS"])
    r = M3 * (y["DSD"] + z["DDS"])
    fx["SDD"] = p + q
    fy["DSD"] = p + r
    fz["DDS"] = q + r
    for f, v in ((fx, x), (fy, y), (fz, z)):
        f["DDD"] = Q * v["DDD"]
    return fx, fy, fz


YZ = ("SS", "SD", "DS", "DD")


def plane_modes(v):
    rows, lanes = v.shape
    nz = pltpu.roll(v, lanes - 1, 1)
    s, d = v + nz, nz - v
    s1, d1 = pltpu.roll(s, rows - 1, 0), pltpu.roll(d, rows - 1, 0)
    return [s + s1, d + d1, s1 - s, d1 - d]


def plane_forces(g):
    B = []
    for zm in (0, 1):
        S, D = g[zm], g[2 + zm]
        B.append((S - D) + pltpu.roll(S + D, 1, 0))
    return (B[0] - B[1]) + pltpu.roll(B[0] + B[1], 1, 1)


def make_kernel(counts, brick, nmat, gl, gm):
    bx, by, bz = counts_brick = brick
    H = max(DEPTHS)
    rounds = len(DEPTHS)
    total = counts[0] * counts[1] * counts[2]
    nfields = [5] + [3 if d == 1 else 5 for d in DEPTHS[1:]]
    YW = by + 8
    ZW = 2 * bz

    def kernel(*refs):
        body, mask, gap, mat, lame, u_out, w_out, gap_out = refs[:8]
        Rs = refs[8 : 8 + rounds]
        Ps = refs[8 + rounds : 8 + 2 * rounds]
        (U, W, N, B, LOW, LL, MM, GA, GT, GR, send, recv, gsend, grecv) = refs[8 + 2 * rounds :]
        me = [lax.axis_index(a) for a in AXES]

        def peer(offset):
            return tuple(lax.rem(me[i] + offset[i] + counts[i], counts[i]) for i in range(3))

        def unravel(j):
            a = j // (counts[1] * counts[2])
            b = (j // counts[2]) % counts[1]
            return (a, b, j % counts[2])

        barrier = pltpu.get_barrier_semaphore()

        @pl.loop(1, total)
        def _(j):
            pl.semaphore_signal(barrier, inc=1, device_id=peer(unravel(j)), device_id_type=MESH)

        lane = lax.broadcasted_iota(jnp.int32, (by, bz), 1)
        lane8 = lax.broadcasted_iota(jnp.int32, (YW, bz), 1)

        def fill(r, fields):
            d = DEPTHS[r]
            for x in range(bx):
                packed = None
                for f, field in enumerate(fields):
                    v = field(x)
                    Rs[r][f, d + x, 8 : 8 + by, :] = v
                    shifted = pltpu.roll(v, 2 * d * f + d, 1)
                    packed = shifted if packed is None else jnp.where(lane >= 2 * d * f, shifted, packed)
                Ps[r][0, d + x, 8 : 8 + by, :] = packed

        def copies(r):
            d = DEPTHS[r]
            for k, (dx, dy, dz) in enumerate(DIRS):
                sx = pl.ds(bx, d) if dx > 0 else pl.ds(d, d if dx else bx)
                tx = pl.ds(0, d) if dx > 0 else (pl.ds(d + bx, d) if dx else pl.ds(d, bx))
                sy = pl.ds(by, 8) if dy > 0 else pl.ds(8, 8 if dy else by)
                ty = pl.ds(0, 8) if dy > 0 else (pl.ds(8 + by, 8) if dy else pl.ds(8, by))
                if dz == 0:
                    src, dst = Rs[r].at[:, sx, sy, :], Rs[r].at[:, tx, ty, :]
                else:
                    src, dst = Ps[r].at[0, sx, sy, :], Ps[r].at[1 if dz > 0 else 2, tx, ty, :]
                yield pltpu.make_async_remote_copy(
                    src_ref=src,
                    dst_ref=dst,
                    send_sem=send.at[r, k],
                    recv_sem=recv.at[r, k],
                    device_id=peer((dx, dy, dz)),
                    device_id_type=MESH,
                )

        def unpack(r, x, f):
            d = DEPTHS[r]
            rows = pl.ds(4, YW)
            own = Rs[r][f, x, rows, :]
            both = jnp.where(lane8 % (2 * d) < d, Ps[r][1, x, rows, :], Ps[r][2, x, rows, :])
            return jnp.concatenate([own, pltpu.roll(both, (bz - (2 * d * f + d)) % bz, 1)], 1)

        top = None
        for m in range(nmat):
            row = lame[m, 0] * gl + lame[m, 1] * gm
            top = row if top is None else jnp.maximum(top, row)
        tau = 1.5 / jnp.full((YW, ZW), 1.0 + 8.0 * top, jnp.float32)

        fill(
            0,
            [
                lambda x: body[0, x],
                lambda x: body[1, x],
                lambda x: body[2, x],
                lambda x: jnp.where(mask[x] > 0, -gap[x], -jnp.inf),
                lambda x: mat[x].astype(jnp.float32),
            ],
        )
        GT[...] = jnp.zeros_like(GT)
        pl.semaphore_wait(barrier, total - 1)

        def settle(x, u, w, low):
            worst = None
            for c in range(3):
                v = u[c] + w[c]
                z = jnp.maximum(v, low) if c == 2 else v
                wc = v - z
                res = u[c] - z
                U[c, x], W[c, x], N[c, x] = u[c], wc, res + wc
                a = jnp.abs(res[:, :bz])
                worst = a if worst is None else jnp.maximum(worst, a)
            inside = jnp.logical_and(x >= H, x < H + bx)
            GA[...] = jnp.maximum(GA[...], jnp.where(inside, worst, 0.0))

        def record(t):
            GT[t : t + 1, :] = jnp.max(GA[4 : 4 + by, :], axis=0, keepdims=True)

        t = 0
        for r, d in enumerate(DEPTHS):
            if r > 0:
                own = (pl.ds(4, by), pl.ds(0, bz))
                fields = [lambda x, c=c: U[c, H + x, own[0], own[1]] for c in range(3)]
                if d > 1:
                    fields += [
                        lambda x: W[2, H + x, own[0], own[1]],
                        lambda x: N[2, H + x, own[0], own[1]],
                    ]
                fill(r, fields)
            for copy in copies(r):
                copy.start()
            for copy in copies(r):
                copy.wait_recv()
            if r == 0:
                GA[...] = jnp.zeros_like(GA)

                @pl.loop(0, bx + 2 * H)
                def _(x):
                    u = []
                    for c in range(3):
                        b = tau * unpack(0, x, c)
                        B[c, x] = b
                        u.append(b)
                    low = unpack(0, x, 3)
                    LOW[x] = low
                    kind = unpack(0, x, 4)
                    first = jnp.zeros_like(kind)
                    shear = jnp.zeros_like(kind)
                    for m in range(nmat):
                        hit = kind == float(m)
                        first = jnp.where(hit, lame[m, 0], first)
                        shear = jnp.where(hit, lame[m, 1], shear)
                    LL[x] = first * (tau * 0.0625)
                    MM[x] = shear * (tau * 0.0625)
                    zero = jnp.zeros_like(kind)
                    settle(x, u, [zero, zero, zero], low)

                record(0)
                t = 1
            else:

                @pl.loop(0, bx + 2 * d)
                def _(x):
                    for c in range(3):
                        U[c, x + H - d] = unpack(r, x, c)
                    if d > 1:
                        W[2, x + H - d] = unpack(r, x, 3)
                        N[2, x + H - d] = unpack(r, x, 4)

            for left in range(d, 0, -1):
                GA[...] = jnp.zeros_like(GA)
                start = H - left

                def step(e, carry):
                    prev, hi = carry
                    cur = [plane_modes(U[c, e + 1]) for c in range(3)]
                    modes = []
                    for c in range(3):
                        m = {}
                        for i, yz in enumerate(YZ):
                            a, b = prev[4 * c + i], cur[c][i]
                            m["D" + yz] = b - a
                            if yz != "SS":
                                m["S" + yz] = a + b
                        modes.append(m)
                    forces = element_modes(modes, LL[e], MM[e])
                    new_hi, u, w = [], [], []
                    for c in range(3):
                        g = []
                        for i, yz in enumerate(YZ):
                            D = forces[c]["D" + yz]
                            h = hi[4 * c + i]
                            if yz == "SS":
                                g.append(h - D)
                                new_hi.append(D)
                            else:
                                S = forces[c]["S" + yz]
                                g.append(h + (S - D))
                                new_hi.append(S + D)
                        F = plane_forces(g)
                        u.append(U[c, e] - ((F - B[c, e]) + tau * N[c, e]))
                        w.append(W[c, e])
                    settle(e, u, w, LOW[e])
                    return [v for c in cur for v in c], new_hi

                zero = jnp.zeros((YW, ZW), jnp.float32)
                carry = ([v for c in range(3) for v in plane_modes(U[c, start])], [zero] * 12)
                lax.fori_loop(start, H + bx - 1 + left, step, carry)
                record(t)
                t += 1

        for c in range(3):
            for x in range(bx):
                u_out[c, x] = U[c, H + x, 4 : 4 + by, :bz]
                w_out[c, x] = W[c, H + x, 4 : 4 + by, :bz]

        @pl.loop(1, total)
        def _(j):
            pltpu.make_async_remote_copy(
                src_ref=GT,
                dst_ref=GR.at[j - 1],
                send_sem=gsend,
                recv_sem=grecv,
                device_id=peer(unravel(j)),
                device_id_type=MESH,
            ).start()

        whole = pltpu.make_async_remote_copy(
            src_ref=GR,
            dst_ref=GR,
            send_sem=gsend,
            recv_sem=grecv,
            device_id=peer((0, 0, 1)),
            device_id_type=MESH,
        )
        whole.wait_recv()
        worst = jnp.maximum(GT[...], jnp.max(GR[...], axis=0))
        for i in range(ITERS):
            gap_out[i] = jnp.max(worst[i : i + 1, :])
        whole.wait_send()
        for r in range(rounds):
            for copy in copies(r):
                copy.wait_send()

    X = bx + 2 * H
    plane = lambda *lead: pltpu.VMEM(lead + (X, YW, ZW), jnp.float32)
    scratch = [
        pltpu.VMEM((n, bx + 2 * d, by + 16, bz), jnp.float32) for n, d in zip(nfields, DEPTHS)
    ]
    scratch += [pltpu.VMEM((3, bx + 2 * d, by + 16, bz), jnp.float32) for d in DEPTHS]
    scratch += [plane(3), plane(3), plane(3), plane(3), plane(), plane(), plane()]
    scratch += [
        pltpu.VMEM((YW, bz), jnp.float32),
        pltpu.VMEM((8, bz), jnp.float32),
        pltpu.VMEM((total - 1, 8, bz), jnp.float32),
        pltpu.SemaphoreType.DMA((rounds, len(DIRS))),
        pltpu.SemaphoreType.DMA((rounds, len(DIRS))),
        pltpu.SemaphoreType.DMA,
        pltpu.SemaphoreType.DMA,
    ]
    return kernel, scratch


def shards(counts, body_load, contact_mask, contact_gap, material_ids, lame_table):
    stiff_lame, stiff_shear = element_tables()
    gl = float(np.max(np.sum(np.abs(stiff_lame), 1)))
    gm = float(np.max(np.sum(np.abs(stiff_shear), 1)))
    kernel, scratch = make_kernel(counts, material_ids.shape, lame_table.shape[0], gl, gm)
    vmem = pl.BlockSpec(memory_space=pltpu.VMEM)
    smem = pl.BlockSpec(memory_space=pltpu.SMEM)
    return pl.pallas_call(
        kernel,
        out_shape=(
            jax.ShapeDtypeStruct(body_load.shape, jnp.float32),
            jax.ShapeDtypeStruct(body_load.shape, jnp.float32),
            jax.ShapeDtypeStruct((ITERS,), jnp.float32),
        ),
        in_specs=[vmem] * 4 + [smem],
        out_specs=(vmem, vmem, smem),
        scratch_shapes=scratch,
        compiler_params=pltpu.CompilerParams(
            collective_id=0, has_side_effects=True, vmem_limit_bytes=48 * 1024 * 1024
        ),
    )(body_load, contact_mask, contact_gap, material_ids, lame_table)


def solution(mesh):
    counts = tuple(mesh.shape[a] for a in AXES)
    in_specs = (
        P(None, "gx", "gy", "gz"),
        P("gx", "gy", "gz"),
        P("gx", "gy", "gz"),
        P("gx", "gy", "gz"),
        P(),
    )
    out_specs = (P(None, "gx", "gy", "gz"), P(None, "gx", "gy", "gz"), P())
    return jax.shard_map(
        functools.partial(shards, counts), mesh=mesh, in_specs=in_specs, out_specs=out_specs, check_vma=False
    )
```

```python
import functools

import jax
import jax.numpy as jnp
import numpy as np
from jax import lax
from jax.experimental import pallas as pl
from jax.experimental.pallas import tpu as pltpu
from jax.sharding import PartitionSpec as P

ITERS = 6
DEPTHS = (3, 2)
AXES = ("gx", "gy", "gz")
MESH = pl.DeviceIdType.MESH


def corner_offsets(a):
    return (a >> 2 & 1, a >> 1 & 1, a & 1)


def element_tables():
    points = np.array([(1.0 - 3.0 ** (-0.5)) / 2.0, (1.0 + 3.0 ** (-0.5)) / 2.0])
    stiff_lame = np.zeros((24, 24))
    stiff_shear = np.zeros((24, 24))
    for p in points:
        for q in points:
            for r in points:
                position = (p, q, r)
                gradients = np.zeros((8, 3))
                for a in range(8):
                    corner = corner_offsets(a)
                    for d in range(3):
                        factor = 1.0
                        for e in range(3):
                            if e == d:
                                factor = factor * (1.0 if corner[e] else -1.0)
                            else:
                                factor = factor * (position[e] if corner[e] else 1.0 - position[e])
                        gradients[a, d] = factor
                for a in range(8):
                    for c in range(3):
                        for b in range(8):
                            for d in range(3):
                                stiff_lame[3 * a + c, 3 * b + d] += 0.125 * gradients[a, c] * gradients[b, d]
                                stiff_shear[3 * a + c, 3 * b + d] += 0.125 * (
                                    float(c == d) * np.dot(gradients[a], gradients[b])
                                    + gradients[a, d] * gradients[b, c]
                                )
    return (stiff_lame, stiff_shear)


def element_modes(m, L, M):
    x, y, z = m
    M2 = M + M
    L3 = L * (1.0 / 3.0)
    M3 = M * (1.0 / 3.0)
    Q = (L + (M2 + M2)) * (1.0 / 9.0)
    s = L * (x["DSS"] + y["SDS"] + z["SSD"])
    fx, fy, fz = {}, {}, {}
    fx["DSS"] = s + M2 * x["DSS"]
    fy["SDS"] = s + M2 * y["SDS"]
    fz["SSD"] = s + M2 * z["SSD"]
    fy["DSS"] = fx["SDS"] = M * (y["DSS"] + x["SDS"])
    fz["DSS"] = fx["SSD"] = M * (z["DSS"] + x["SSD"])
    fz["SDS"] = fy["SSD"] = M * (z["SDS"] + y["SSD"])
    ax = L3 * (y["DDS"] + z["DSD"])
    ay = L3 * (x["DDS"] + z["SDD"])
    az = L3 * (x["DSD"] + y["SDD"])
    fx["DDS"] = ay + M * x["DDS"]
    fx["DSD"] = az + M * x["DSD"]
    fy["DDS"] = ax + M * y["DDS"]
    fy["SDD"] = az + M * y["SDD"]
    fz["DSD"] = ax + M * z["DSD"]
    fz["SDD"] = ay + M * z["SDD"]
    p = M3 * (y["DSD"] + x["SDD"])
    q = M3 * (x["SDD"] + z["DDS"])
    r = M3 * (y["DSD"] + z["DDS"])
    fx["SDD"] = p + q
    fy["DSD"] = p + r
    fz["DDS"] = q + r
    for f, v in ((fx, x), (fy, y), (fz, z)):
        f["DDD"] = Q * v["DDD"]
    return fx, fy, fz


YZ = ("SS", "SD", "DS", "DD")


def plane_modes(v):
    rows, lanes = v.shape
    nz = pltpu.roll(v, lanes - 1, 1)
    s, d = v + nz, nz - v
    s1, d1 = pltpu.roll(s, rows - 1, 0), pltpu.roll(d, rows - 1, 0)
    return [s + s1, d + d1, s1 - s, d1 - d]


def plane_forces(g):
    B = []
    for zm in (0, 1):
        S, D = g[zm], g[2 + zm]
        B.append((S - D) + pltpu.roll(S + D, 1, 0))
    return (B[0] - B[1]) + pltpu.roll(B[0] + B[1], 1, 1)


def make_kernel(counts, brick, nmat, gl, gm):
    bx, by, bz = brick
    H = max(DEPTHS)
    rounds = len(DEPTHS)
    total = counts[0] * counts[1] * counts[2]
    nfields = [5] + [3] * (rounds - 1)
    YW = by + 8
    ZW = 2 * bz
    slots = min(counts[0], 3)
    xdirs = (0, 1) if counts[0] == 2 else (0, 1, -1)
    dirs = [(dx, dy, dz) for dx in xdirs for dy in (-1, 0, 1) for dz in (-1, 0, 1)][0:]
    dirs = [k for k in dirs if k != (0, 0, 0)]
    dirs.sort(key=lambda k: -sum(abs(a) for a in k))
    ytiles = [-(-n * d // 8) * 8 for n, d in zip(nfields, DEPTHS)]
    group = [max(1, bz // (2 * d * n)) for n, d in zip(nfields, DEPTHS)]
    ztiles = [-(-bx // g) for g in group]

    def kernel(*refs):
        body, mask_in, gap_in, mat_in, lame, u_out, w_out, gap_out = refs[:8]
        Rs, YSs, YBs, ZBs = (refs[8 + i * rounds : 8 + (i + 1) * rounds] for i in range(4))
        (U, W, N, B, LOW, LL, MM, GA, GT, GR, mask, gap, mat, send, recv, gsend, grecv, isem) = refs[8 + 4 * rounds :]
        me = [lax.axis_index(a) for a in AXES]
        around = [[lax.rem(me[i] + k, counts[i]) for k in range(counts[i])] for i in range(3)]

        def peer(offset):
            return tuple(around[i][offset[i] % counts[i]] for i in range(3))

        def everyone(act):
            if total <= 64:
                for j in range(1, total):
                    a, b = j // (counts[1] * counts[2]), (j // counts[2]) % counts[1]
                    act(j - 1, peer((a, b, j % counts[2])))
            else:

                @pl.loop(1, total)
                def _(j):
                    step = (j // (counts[1] * counts[2]), (j // counts[2]) % counts[1], j % counts[2])
                    act(j - 1, tuple(lax.rem(me[i] + step[i], counts[i]) for i in range(3)))

        barrier = pltpu.get_barrier_semaphore()
        loads = [
            pltpu.make_async_copy(body, Rs[0].at[pl.ds(0, 3), pl.ds(0, bx)], isem.at[0]),
            pltpu.make_async_copy(mask_in, mask, isem.at[1]),
            pltpu.make_async_copy(gap_in, gap, isem.at[2]),
            pltpu.make_async_copy(mat_in, mat, isem.at[3]),
        ]
        for load in loads:
            load.start()
        everyone(lambda j, who: pl.semaphore_signal(barrier, inc=1, device_id=who, device_id_type=MESH))

        lane = lax.broadcasted_iota(jnp.int32, (by, bz), 1)
        lane8 = lax.broadcasted_iota(jnp.int32, (YW, bz), 1)

        def fill(r):
            d, n = DEPTHS[r], nfields[r]
            for tile in range(ztiles[r]):
                packed = None
                for x in range(tile * group[r], min(bx, (tile + 1) * group[r])):
                    for f in range(n):
                        v = Rs[r][f, x]
                        YSs[r][0, x, f * d : f * d + d, :] = v[by - d :]
                        YSs[r][1, x, f * d : f * d + d, :] = v[:d]
                        at = 2 * d * ((x - tile * group[r]) * n + f)
                        shifted = pltpu.roll(v, (at + d) % bz, 1)
                        packed = shifted if packed is None else jnp.where(lane >= at, shifted, packed)
                ZBs[r][0, 0, tile, 8 : 8 + by, :] = packed

        def copies(r):
            for k, (dx, dy, dz) in enumerate(dirs):
                slot = 0 if dx == 0 else (1 if dx < 0 or counts[0] == 2 else 2)
                planes = pl.ds(slot * bx, bx)
                if dz != 0:
                    sy = pl.ds(by, 8) if dy > 0 else pl.ds(8, 8 if dy else by)
                    ty = pl.ds(0, 8) if dy > 0 else (pl.ds(8 + by, 8) if dy else pl.ds(8, by))
                    src = ZBs[r].at[0, 0, :, sy, :]
                    dst = ZBs[r].at[1 if dz > 0 else 2, slot, :, ty, :]
                elif dy != 0:
                    side = 0 if dy > 0 else 1
                    src, dst = YSs[r].at[side], YBs[r].at[side, planes]
                else:
                    src, dst = Rs[r].at[:, pl.ds(0, bx)], Rs[r].at[:, planes]
                yield pltpu.make_async_remote_copy(
                    src_ref=src,
                    dst_ref=dst,
                    send_sem=send.at[r, k],
                    recv_sem=recv.at[r, k],
                    device_id=peer((dx, dy, dz)),
                    device_id_type=MESH,
                )

        def unpack(r, targets):
            d, n = DEPTHS[r], nfields[r]
            for x in range(H - d, H + bx + d):
                at = (x - H) % (slots * bx)
                slot, p = at // bx, at % bx
                tile = p // group[r]
                rows = pl.ds(4, YW)
                both = jnp.where(
                    lane8 % (2 * d) < d, ZBs[r][1, slot, tile, rows, :], ZBs[r][2, slot, tile, rows, :]
                )
                for f, put in enumerate(targets):
                    o = put(x)
                    if r == 0 or slot != 0:
                        o[4 : 4 + by, :bz] = Rs[r][f, at]
                    o[4 - d : 4, :bz] = YBs[r][0, at, f * d : f * d + d, :]
                    o[4 + by : 4 + by + d, :bz] = YBs[r][1, at, f * d : f * d + d, :]
                    shift = 2 * d * ((p - tile * group[r]) * n + f) + d
                    o[:, bz:] = pltpu.roll(both, (bz - shift) % bz, 1)

        top = None
        for m in range(nmat):
            row = lame[0, m] * gl + lame[1, m] * gm
            top = row if top is None else jnp.maximum(top, row)
        tau = 1.5 / jnp.full((YW, ZW), 1.0 + 8.0 * top, jnp.float32)

        for load in loads:
            load.wait()
        for x in range(bx):
            Rs[0][3, x] = jnp.where(mask[x] > 0, -gap[x], -jnp.inf)
            Rs[0][4, x] = mat[x].astype(jnp.float32)
        fill(0)
        GT[...] = jnp.zeros_like(GT)
        pl.semaphore_wait(barrier, total - 1)

        def settle(x, u, w, low):
            worst = None
            for c in range(3):
                v = u[c] + w[c]
                z = jnp.maximum(v, low) if c == 2 else v
                wc = v - z
                res = u[c] - z
                W[c, x], N[c, x] = wc, res + wc
                a = jnp.abs(res[:, :bz])
                worst = a if worst is None else jnp.maximum(worst, a)
            inside = jnp.logical_and(x >= H, x < H + bx)
            GA[...] = jnp.maximum(GA[...], jnp.where(inside, worst, 0.0))

        def record(t):
            GT[t : t + 1, :] = jnp.max(GA[4 : 4 + by, :], axis=0, keepdims=True)
            GA[...] = jnp.zeros_like(GA)

        GA[...] = jnp.zeros_like(GA)
        t = 0
        for r, d in enumerate(DEPTHS):
            if r > 0:
                for c in range(3):
                    for x in range(bx):
                        Rs[r][c, x] = U[c, H + x, 4 : 4 + by, :bz]
                fill(r)
            for copy in copies(r):
                copy.start()
            for copy in copies(r):
                copy.wait_recv()
            if r == 0:
                unpack(0, [lambda x, c=c: B.at[c, x] for c in range(3)] + [lambda x: LOW.at[x], lambda x: LL.at[x]])

                @pl.loop(0, bx + 2 * H)
                def _(x):
                    u = []
                    for c in range(3):
                        b = tau * B[c, x]
                        B[c, x] = b
                        U[c, x] = b
                        u.append(b)
                    kind = LL[x]
                    first = jnp.zeros_like(kind)
                    shear = jnp.zeros_like(kind)
                    for m in range(nmat):
                        hit = kind == float(m)
                        first = jnp.where(hit, lame[0, m], first)
                        shear = jnp.where(hit, lame[1, m], shear)
                    LL[x] = first * (tau * 0.0625)
                    MM[x] = shear * (tau * 0.0625)
                    zero = jnp.zeros_like(kind)
                    settle(x, u, [zero, zero, zero], LOW[x])

            else:
                unpack(r, [lambda x, c=c: U.at[c, x] for c in range(3)])

                @pl.loop(H - d + 1, H + bx + d - 1)
                def _(x):
                    settle(x, [U[c, x] for c in range(3)], [W[c, x] for c in range(3)], LOW[x])

            record(t)
            t += 1
            for left in range(d, 0, -1):
                start = H - left
                final = left > 1 or r == rounds - 1

                def step(e, carry):
                    prev, hi = carry
                    cur = [plane_modes(U[c, e + 1]) for c in range(3)]
                    modes = []
                    for c in range(3):
                        m = {}
                        for i, yz in enumerate(YZ):
                            a, b = prev[4 * c + i], cur[c][i]
                            m["D" + yz] = b - a
                            if yz != "SS":
                                m["S" + yz] = a + b
                        modes.append(m)
                    forces = element_modes(modes, LL[e], MM[e])
                    new_hi, u = [], []
                    for c in range(3):
                        g = []
                        for i, yz in enumerate(YZ):
                            D = forces[c]["D" + yz]
                            h = hi[4 * c + i]
                            if yz == "SS":
                                g.append(h - D)
                                new_hi.append(D)
                            else:
                                S = forces[c]["S" + yz]
                                g.append(h + (S - D))
                                new_hi.append(S + D)
                        F = plane_forces(g)
                        u.append(U[c, e] - ((F - B[c, e]) + tau * N[c, e]))
                        U[c, e] = u[c]
                    if final:
                        settle(e, u, [W[c, e] for c in range(3)], LOW[e])
                    return [v for c in cur for v in c], new_hi

                zero = jnp.zeros((YW, ZW), jnp.float32)
                carry = ([v for c in range(3) for v in plane_modes(U[c, start])], [zero] * 12)
                lax.fori_loop(start, H + bx - 1 + left, step, carry, unroll=True)
                if final:
                    record(t)
                    t += 1

        def spread(j, who):
            return pltpu.make_async_remote_copy(
                src_ref=GT,
                dst_ref=GR.at[j],
                send_sem=gsend,
                recv_sem=grecv,
                device_id=who,
                device_id_type=MESH,
            )

        everyone(lambda j, who: spread(j, who).start())
        for c in range(3):
            for x in range(bx):
                u_out[c, x] = U[c, H + x, 4 : 4 + by, :bz]
                w_out[c, x] = W[c, H + x, 4 : 4 + by, :bz]
        for r in range(rounds):
            for copy in copies(r):
                copy.wait_send()
        whole = pltpu.make_async_remote_copy(
            src_ref=GR,
            dst_ref=GR,
            send_sem=gsend,
            recv_sem=grecv,
            device_id=peer((0, 0, 1)),
            device_id_type=MESH,
        )
        whole.wait_recv()
        worst = jnp.maximum(GT[...], jnp.max(GR[...], axis=0))
        for i in range(ITERS):
            gap_out[i] = jnp.max(worst[i : i + 1, :])
        whole.wait_send()

    X = bx + 2 * H
    buffer = lambda *dims: pltpu.VMEM(dims, jnp.float32)
    scratch = [buffer(n, slots * bx, by, bz) for n in nfields]
    scratch += [buffer(2, bx, rows, bz) for rows in ytiles]
    scratch += [buffer(2, slots * bx, rows, bz) for rows in ytiles]
    scratch += [buffer(3, slots, tiles, by + 16, bz) for tiles in ztiles]
    scratch += [buffer(3, X, YW, ZW)] * 4 + [buffer(X, YW, ZW)] * 3
    scratch += [
        buffer(YW, bz),
        buffer(8, bz),
        buffer(total - 1, 8, bz),
        pltpu.VMEM((bx, by, bz), jnp.int32),
        buffer(bx, by, bz),
        pltpu.VMEM((bx, by, bz), jnp.int32),
        pltpu.SemaphoreType.DMA((rounds, len(dirs))),
        pltpu.SemaphoreType.DMA((rounds, len(dirs))),
        pltpu.SemaphoreType.DMA,
        pltpu.SemaphoreType.DMA,
        pltpu.SemaphoreType.DMA((4,)),
    ]
    return kernel, scratch


def shards(counts, body_load, contact_mask, contact_gap, material_ids, lame_table):
    stiff_lame, stiff_shear = element_tables()
    gl = float(np.max(np.sum(np.abs(stiff_lame), 1)))
    gm = float(np.max(np.sum(np.abs(stiff_shear), 1)))
    kernel, scratch = make_kernel(counts, material_ids.shape, lame_table.shape[0], gl, gm)
    vmem = pl.BlockSpec(memory_space=pltpu.VMEM)
    anywhere = pl.BlockSpec(memory_space=pltpu.HBM)
    smem = pl.BlockSpec(memory_space=pltpu.SMEM)
    return pl.pallas_call(
        kernel,
        out_shape=(
            jax.ShapeDtypeStruct(body_load.shape, jnp.float32),
            jax.ShapeDtypeStruct(body_load.shape, jnp.float32),
            jax.ShapeDtypeStruct((ITERS,), jnp.float32),
        ),
        in_specs=[anywhere] * 4 + [smem],
        out_specs=(vmem, vmem, smem),
        scratch_shapes=scratch,
        compiler_params=pltpu.CompilerParams(
            collective_id=0, has_side_effects=True, vmem_limit_bytes=62 * 1024 * 1024
        ),
    )(body_load, contact_mask, contact_gap, material_ids, lame_table.T)


def solution(mesh):
    counts = tuple(mesh.shape[a] for a in AXES)
    in_specs = (
        P(None, "gx", "gy", "gz"),
        P("gx", "gy", "gz"),
        P("gx", "gy", "gz"),
        P("gx", "gy", "gz"),
        P(),
    )
    out_specs = (P(None, "gx", "gy", "gz"), P(None, "gx", "gy", "gz"), P())
    return jax.shard_map(
        functools.partial(shards, counts), mesh=mesh, in_specs=in_specs, out_specs=out_specs, check_vma=False
    )
```

```python
import functools

import jax
import jax.numpy as jnp
import numpy as np
from jax import lax
from jax.experimental import pallas as pl
from jax.experimental.pallas import tpu as pltpu
from jax.sharding import PartitionSpec as P

ITERS = 6
DEPTHS = (3, 2)
AXES = ("gx", "gy", "gz")
MESH = pl.DeviceIdType.MESH


def corner_offsets(a):
    return (a >> 2 & 1, a >> 1 & 1, a & 1)


def element_tables():
    points = np.array([(1.0 - 3.0 ** (-0.5)) / 2.0, (1.0 + 3.0 ** (-0.5)) / 2.0])
    stiff_lame = np.zeros((24, 24))
    stiff_shear = np.zeros((24, 24))
    for p in points:
        for q in points:
            for r in points:
                position = (p, q, r)
                gradients = np.zeros((8, 3))
                for a in range(8):
                    corner = corner_offsets(a)
                    for d in range(3):
                        factor = 1.0
                        for e in range(3):
                            if e == d:
                                factor = factor * (1.0 if corner[e] else -1.0)
                            else:
                                factor = factor * (position[e] if corner[e] else 1.0 - position[e])
                        gradients[a, d] = factor
                for a in range(8):
                    for c in range(3):
                        for b in range(8):
                            for d in range(3):
                                stiff_lame[3 * a + c, 3 * b + d] += 0.125 * gradients[a, c] * gradients[b, d]
                                stiff_shear[3 * a + c, 3 * b + d] += 0.125 * (
                                    float(c == d) * np.dot(gradients[a], gradients[b])
                                    + gradients[a, d] * gradients[b, c]
                                )
    return (stiff_lame, stiff_shear)


def element_modes(m, L, M):
    x, y, z = m
    M2 = M + M
    L3 = L * (1.0 / 3.0)
    M3 = M * (1.0 / 3.0)
    Q = (L + (M2 + M2)) * (1.0 / 9.0)
    s = L * (x["DSS"] + y["SDS"] + z["SSD"])
    fx, fy, fz = {}, {}, {}
    fx["DSS"] = s + M2 * x["DSS"]
    fy["SDS"] = s + M2 * y["SDS"]
    fz["SSD"] = s + M2 * z["SSD"]
    fy["DSS"] = fx["SDS"] = M * (y["DSS"] + x["SDS"])
    fz["DSS"] = fx["SSD"] = M * (z["DSS"] + x["SSD"])
    fz["SDS"] = fy["SSD"] = M * (z["SDS"] + y["SSD"])
    ax = L3 * (y["DDS"] + z["DSD"])
    ay = L3 * (x["DDS"] + z["SDD"])
    az = L3 * (x["DSD"] + y["SDD"])
    fx["DDS"] = ay + M * x["DDS"]
    fx["DSD"] = az + M * x["DSD"]
    fy["DDS"] = ax + M * y["DDS"]
    fy["SDD"] = az + M * y["SDD"]
    fz["DSD"] = ax + M * z["DSD"]
    fz["SDD"] = ay + M * z["SDD"]
    p = M3 * (y["DSD"] + x["SDD"])
    q = M3 * (x["SDD"] + z["DDS"])
    r = M3 * (y["DSD"] + z["DDS"])
    fx["SDD"] = p + q
    fy["DSD"] = p + r
    fz["DDS"] = q + r
    for f, v in ((fx, x), (fy, y), (fz, z)):
        f["DDD"] = Q * v["DDD"]
    return fx, fy, fz


YZ = ("SS", "SD", "DS", "DD")


def plane_modes(v):
    rows, lanes = v.shape
    nz = pltpu.roll(v, lanes - 1, 1)
    s, d = v + nz, nz - v
    s1, d1 = pltpu.roll(s, rows - 1, 0), pltpu.roll(d, rows - 1, 0)
    return [s + s1, d + d1, s1 - s, d1 - d]


def plane_forces(g):
    B = []
    for zm in (0, 1):
        S, D = g[zm], g[2 + zm]
        B.append((S - D) + pltpu.roll(S + D, 1, 0))
    return (B[0] - B[1]) + pltpu.roll(B[0] + B[1], 1, 1)


def make_kernel(counts, brick, nmat, gl, gm):
    bx, by, bz = brick
    H = max(DEPTHS)
    rounds = len(DEPTHS)
    total = counts[0] * counts[1] * counts[2]
    nfields = [5] + [3] * (rounds - 1)
    YW = by + 8
    ZW = 2 * bz
    slots = min(counts[0], 3)
    xdirs = (0, 1) if counts[0] == 2 else (0, 1, -1)
    dirs = [(dx, dy, dz) for dx in xdirs for dy in (-1, 0, 1) for dz in (-1, 0, 1)][0:]
    dirs = [k for k in dirs if k != (0, 0, 0)]
    dirs.sort(key=lambda k: -sum(abs(a) for a in k))
    ytiles = [-(-n * d // 8) * 8 for n, d in zip(nfields, DEPTHS)]
    group = [max(1, bz // (2 * d * n)) for n, d in zip(nfields, DEPTHS)]
    ztiles = [-(-bx // g) for g in group]

    def kernel(*refs):
        body, mask_in, gap_in, mat_in, lame_in, u_out, w_out, gap_out = refs[:8]
        Rs, YSs, YBs, ZBs = (refs[8 + i * rounds : 8 + (i + 1) * rounds] for i in range(4))
        (U, W, N, B, LOW, LL, MM, GA, GT, GR, mask, gap, mat, lame, send, recv, gsend, grecv, isem) = refs[8 + 4 * rounds :]
        me = [lax.axis_index(a) for a in AXES]
        around = [[lax.rem(me[i] + k, counts[i]) for k in range(counts[i])] for i in range(3)]

        def peer(offset):
            return tuple(around[i][offset[i] % counts[i]] for i in range(3))

        def everyone(act):
            if total <= 64:
                for j in range(total - 1, 0, -1):
                    a, b = j // (counts[1] * counts[2]), (j // counts[2]) % counts[1]
                    act(j - 1, peer((a, b, j % counts[2])))
            else:

                @pl.loop(1, total)
                def _(j):
                    step = (j // (counts[1] * counts[2]), (j // counts[2]) % counts[1], j % counts[2])
                    act(j - 1, tuple(lax.rem(me[i] + step[i], counts[i]) for i in range(3)))

        barrier = pltpu.get_barrier_semaphore()
        loads = [
            pltpu.make_async_copy(body, Rs[0].at[pl.ds(0, 3), pl.ds(0, bx)], isem.at[0]),
            pltpu.make_async_copy(mask_in, mask, isem.at[1]),
            pltpu.make_async_copy(gap_in, gap, isem.at[2]),
            pltpu.make_async_copy(mat_in, mat, isem.at[3]),
            pltpu.make_async_copy(lame_in, lame, isem.at[4]),
        ]
        for load in loads:
            load.start()
        everyone(lambda j, who: pl.semaphore_signal(barrier, inc=1, device_id=who, device_id_type=MESH))

        lane = lax.broadcasted_iota(jnp.int32, (by, bz), 1)
        lane8 = lax.broadcasted_iota(jnp.int32, (YW, bz), 1)

        def fill(r):
            d, n = DEPTHS[r], nfields[r]
            for tile in range(ztiles[r]):
                packed = None
                for x in range(tile * group[r], min(bx, (tile + 1) * group[r])):
                    for f in range(n):
                        v = Rs[r][f, x]
                        YSs[r][0, x, f * d : f * d + d, :] = v[by - d :]
                        YSs[r][1, x, f * d : f * d + d, :] = v[:d]
                        at = 2 * d * ((x - tile * group[r]) * n + f)
                        shifted = pltpu.roll(v, (at + d) % bz, 1)
                        packed = shifted if packed is None else jnp.where(lane >= at, shifted, packed)
                ZBs[r][0, 0, tile, 8 : 8 + by, :] = packed

        def copies(r):
            for k, (dx, dy, dz) in enumerate(dirs):
                slot = 0 if dx == 0 else (1 if dx < 0 or counts[0] == 2 else 2)
                planes = pl.ds(slot * bx, bx)
                if dz != 0:
                    sy = pl.ds(by, 8) if dy > 0 else pl.ds(8, 8 if dy else by)
                    ty = pl.ds(0, 8) if dy > 0 else (pl.ds(8 + by, 8) if dy else pl.ds(8, by))
                    src = ZBs[r].at[0, 0, :, sy, :]
                    dst = ZBs[r].at[1 if dz > 0 else 2, slot, :, ty, :]
                elif dy != 0:
                    side = 0 if dy > 0 else 1
                    src, dst = YSs[r].at[side], YBs[r].at[side, planes]
                else:
                    src, dst = Rs[r].at[:, pl.ds(0, bx)], Rs[r].at[:, planes]
                yield pltpu.make_async_remote_copy(
                    src_ref=src,
                    dst_ref=dst,
                    send_sem=send.at[r, k],
                    recv_sem=recv.at[r, k],
                    device_id=peer((dx, dy, dz)),
                    device_id_type=MESH,
                )

        def unpack(r, targets):
            d, n = DEPTHS[r], nfields[r]
            for x in range(H - d, H + bx + d):
                at = (x - H) % (slots * bx)
                slot, p = at // bx, at % bx
                tile = p // group[r]
                rows = pl.ds(4, YW)
                both = jnp.where(
                    lane8 % (2 * d) < d, ZBs[r][1, slot, tile, rows, :], ZBs[r][2, slot, tile, rows, :]
                )
                for f, put in enumerate(targets):
                    o = put(x)
                    if r == 0 or slot != 0:
                        o[4 : 4 + by, :bz] = Rs[r][f, at]
                    o[4 - d : 4, :bz] = YBs[r][0, at, f * d : f * d + d, :]
                    o[4 + by : 4 + by + d, :bz] = YBs[r][1, at, f * d : f * d + d, :]
                    shift = 2 * d * ((p - tile * group[r]) * n + f) + d
                    o[:, bz:] = pltpu.roll(both, (bz - shift) % bz, 1)

        for load in loads:
            load.wait()
        top = None
        for m in range(nmat):
            row = lame[0, m] * gl + lame[1, m] * gm
            top = row if top is None else jnp.maximum(top, row)
        tau = 1.5 / jnp.full((YW, ZW), 1.0 + 8.0 * top, jnp.float32)

        for x in range(bx):
            Rs[0][3, x] = jnp.where(mask[x] > 0, -gap[x], -jnp.inf)
            Rs[0][4, x] = mat[x].astype(jnp.float32)
        fill(0)
        GT[...] = jnp.zeros_like(GT)
        pl.semaphore_wait(barrier, total - 1)

        def settle(x, u, w, low):
            worst = None
            for c in range(3):
                v = u[c] + w[c]
                z = jnp.maximum(v, low) if c == 2 else v
                wc = v - z
                res = u[c] - z
                W[c, x], N[c, x] = wc, res + wc
                a = jnp.abs(res[:, :bz])
                worst = a if worst is None else jnp.maximum(worst, a)
            inside = jnp.logical_and(x >= H, x < H + bx)
            GA[...] = jnp.maximum(GA[...], jnp.where(inside, worst, 0.0))

        def record(t):
            GT[t : t + 1, :] = jnp.max(GA[4 : 4 + by, :], axis=0, keepdims=True)
            GA[...] = jnp.zeros_like(GA)

        GA[...] = jnp.zeros_like(GA)
        t = 0
        for r, d in enumerate(DEPTHS):
            if r > 0:
                for c in range(3):
                    for x in range(bx):
                        Rs[r][c, x] = U[c, H + x, 4 : 4 + by, :bz]
                fill(r)
            for copy in copies(r):
                copy.start()
            for copy in copies(r):
                copy.wait_recv()
            if r == 0:
                unpack(0, [lambda x, c=c: B.at[c, x] for c in range(3)] + [lambda x: LOW.at[x], lambda x: LL.at[x]])

                @pl.loop(0, bx + 2 * H)
                def _(x):
                    u = []
                    for c in range(3):
                        b = tau * B[c, x]
                        B[c, x] = b
                        U[c, x] = b
                        u.append(b)
                    kind = LL[x]
                    first = jnp.zeros_like(kind)
                    shear = jnp.zeros_like(kind)
                    for m in range(nmat):
                        hit = kind == float(m)
                        first = jnp.where(hit, lame[0, m], first)
                        shear = jnp.where(hit, lame[1, m], shear)
                    LL[x] = first * (tau * 0.0625)
                    MM[x] = shear * (tau * 0.0625)
                    zero = jnp.zeros_like(kind)
                    settle(x, u, [zero, zero, zero], LOW[x])

            else:
                unpack(r, [lambda x, c=c: U.at[c, x] for c in range(3)])

                @pl.loop(H - d + 1, H + bx + d - 1)
                def _(x):
                    settle(x, [U[c, x] for c in range(3)], [W[c, x] for c in range(3)], LOW[x])

            record(t)
            t += 1
            for left in range(d, 0, -1):
                start = H - left
                final = left > 1 or r == rounds - 1

                def step(e, carry):
                    prev, hi = carry
                    cur = [plane_modes(U[c, e + 1]) for c in range(3)]
                    modes = []
                    for c in range(3):
                        m = {}
                        for i, yz in enumerate(YZ):
                            a, b = prev[4 * c + i], cur[c][i]
                            m["D" + yz] = b - a
                            if yz != "SS":
                                m["S" + yz] = a + b
                        modes.append(m)
                    forces = element_modes(modes, LL[e], MM[e])
                    new_hi, u = [], []
                    for c in range(3):
                        g = []
                        for i, yz in enumerate(YZ):
                            D = forces[c]["D" + yz]
                            h = hi[4 * c + i]
                            if yz == "SS":
                                g.append(h - D)
                                new_hi.append(D)
                            else:
                                S = forces[c]["S" + yz]
                                g.append(h + (S - D))
                                new_hi.append(S + D)
                        F = plane_forces(g)
                        u.append(U[c, e] - ((F - B[c, e]) + tau * N[c, e]))
                        U[c, e] = u[c]
                    if final:
                        settle(e, u, [W[c, e] for c in range(3)], LOW[e])
                    return [v for c in cur for v in c], new_hi

                zero = jnp.zeros((YW, ZW), jnp.float32)
                carry = ([v for c in range(3) for v in plane_modes(U[c, start])], [zero] * 12)
                lax.fori_loop(start, H + bx - 1 + left, step, carry, unroll=True)
                if final:
                    record(t)
                    t += 1

        def spread(j, who):
            return pltpu.make_async_remote_copy(
                src_ref=GT,
                dst_ref=GR.at[j],
                send_sem=gsend,
                recv_sem=grecv,
                device_id=who,
                device_id_type=MESH,
            )

        everyone(lambda j, who: spread(j, who).start())
        for c in range(3):
            for x in range(bx):
                u_out[c, x] = U[c, H + x, 4 : 4 + by, :bz]
                w_out[c, x] = W[c, H + x, 4 : 4 + by, :bz]
        for r in range(rounds):
            for copy in copies(r):
                copy.wait_send()
        whole = pltpu.make_async_remote_copy(
            src_ref=GR,
            dst_ref=GR,
            send_sem=gsend,
            recv_sem=grecv,
            device_id=peer((0, 0, 1)),
            device_id_type=MESH,
        )
        whole.wait_recv()
        worst = jnp.maximum(GT[...], jnp.max(GR[...], axis=0))
        for i in range(ITERS):
            gap_out[i] = jnp.max(worst[i : i + 1, :])
        whole.wait_send()

    X = bx + 2 * H
    buffer = lambda *dims: pltpu.VMEM(dims, jnp.float32)
    scratch = [buffer(n, slots * bx, by, bz) for n in nfields]
    scratch += [buffer(2, bx, rows, bz) for rows in ytiles]
    scratch += [buffer(2, slots * bx, rows, bz) for rows in ytiles]
    scratch += [buffer(3, slots, tiles, by + 16, bz) for tiles in ztiles]
    scratch += [buffer(3, X, YW, ZW)] * 4 + [buffer(X, YW, ZW)] * 3
    scratch += [
        buffer(YW, bz),
        buffer(8, bz),
        buffer(total - 1, 8, bz),
        pltpu.VMEM((bx, by, bz), jnp.int32),
        buffer(bx, by, bz),
        pltpu.VMEM((bx, by, bz), jnp.int32),
        pltpu.SMEM((2, nmat), jnp.float32),
        pltpu.SemaphoreType.DMA((rounds, len(dirs))),
        pltpu.SemaphoreType.DMA((rounds, len(dirs))),
        pltpu.SemaphoreType.DMA,
        pltpu.SemaphoreType.DMA,
        pltpu.SemaphoreType.DMA((5,)),
    ]
    return kernel, scratch


def shards(counts, body_load, contact_mask, contact_gap, material_ids, lame_table):
    stiff_lame, stiff_shear = element_tables()
    gl = float(np.max(np.sum(np.abs(stiff_lame), 1)))
    gm = float(np.max(np.sum(np.abs(stiff_shear), 1)))
    kernel, scratch = make_kernel(counts, material_ids.shape, lame_table.shape[0], gl, gm)
    vmem = pl.BlockSpec(memory_space=pltpu.VMEM)
    anywhere = pl.BlockSpec(memory_space=pltpu.HBM)
    smem = pl.BlockSpec(memory_space=pltpu.SMEM)
    return pl.pallas_call(
        kernel,
        out_shape=(
            jax.ShapeDtypeStruct(body_load.shape, jnp.float32),
            jax.ShapeDtypeStruct(body_load.shape, jnp.float32),
            jax.ShapeDtypeStruct((ITERS,), jnp.float32),
        ),
        in_specs=[anywhere] * 5,
        out_specs=(vmem, vmem, smem),
        scratch_shapes=scratch,
        compiler_params=pltpu.CompilerParams(
            collective_id=0, has_side_effects=True, vmem_limit_bytes=62 * 1024 * 1024
        ),
    )(body_load, contact_mask, contact_gap, material_ids, lame_table.T)


def solution(mesh):
    counts = tuple(mesh.shape[a] for a in AXES)
    in_specs = (
        P(None, "gx", "gy", "gz"),
        P("gx", "gy", "gz"),
        P("gx", "gy", "gz"),
        P("gx", "gy", "gz"),
        P(),
    )
    out_specs = (P(None, "gx", "gy", "gz"), P(None, "gx", "gy", "gz"), P())
    return jax.shard_map(
        functools.partial(shards, counts), mesh=mesh, in_specs=in_specs, out_specs=out_specs, check_vma=False
    )
```
